128 devices in a mesh: dp: 16 (over y_hi, x, core), mp: 8 (over z, y_lo).
Axes of the slice: x: 4, y: 4 (y_hi: 2, y_lo: 2; y = y_hi * 2 + y_lo), z: 4, core: 2. Of those that a mesh axis runs over, the one named last changes fastest.
Arguments:
- hidden_states: bfloat16 [65536, 4096], P('dp', 'mp'), may hold values from -1 to 1
- factor_values: bfloat16 [65536, 128], P('dp', 'mp'), may hold values from 0.029907227 to 0.13964844
- class_ids: int32 [65536, 128], P('dp', 'mp'), may hold values from 0 to 128255, as said below
- centers: int32 [3], replicated, may hold values from 0 to 65535
Outputs:
- min_distance: float32 [65536], P(('dp', 'mp'))
- weight_means: float32 [3], replicated
The draws below stay inside these ranges and needn't reach their ends.
Inputs may be any that keep to these rules, and one draw needn't show every extreme that they name: `centers`: each value is a sample index. `class_ids`: entries k * 16 to (k + 1) * 16 - 1 of a row hold distinct classes of the k-th of 8 equal ranges of the vocabulary.
All inputs are finite; a program needn't handle non-finite values.
Results may differ from the reference program's by a relative error of at most 0.00095.
Values may be sent and summed in bfloat16 or wider, within the bound.
A program may use at most 64 MiB of HBM per device.

```python
import jax
import jax.numpy as jnp
from jax import lax

D = 4096
VOCAB = 128256
K_LOC = 16
STEPS = 3
SAMP_DEV = 512
TOPK = 128
POOL = 65536


def draw_hidden_states(key, part):
    key_shared, key_noise = jax.random.split(key, 2)
    shared = jax.random.normal(key_shared, (1, D), jnp.float32)
    noise = jax.random.normal(key_noise, (POOL, D), jnp.float32)
    base = 0.7 * shared + 0.7 * noise
    return jnp.clip(base / jnp.sqrt(jnp.float32(D)), -1.0, 1.0).astype(jnp.bfloat16)


def draw_class_ids(key, part):
    nblk = TOPK // K_LOC
    span = VOCAB // nblk
    stride = span // K_LOC
    key_order, key_pick, key_near, key_far = jax.random.split(key, 4)
    scores = jax.random.randint(key_order, (POOL, nblk, K_LOC), 0, 1 << 20) * K_LOC + jnp.arange(K_LOC, dtype=jnp.int32)
    slots = jnp.argsort(scores, axis=-1, stable=True).astype(jnp.int32)
    pick = jax.random.randint(key_pick, (POOL, nblk, K_LOC), 0, 4)
    near = jax.random.randint(key_near, (POOL, nblk, K_LOC), 0, 4)
    far = jax.random.randint(key_far, (POOL, nblk, K_LOC), 0, stride)
    offset = jnp.where(pick > 0, near, far)
    base = (jnp.arange(nblk, dtype=jnp.int32) * span).reshape(1, nblk, 1)
    ids = base + slots * stride + offset
    return ids.reshape(POOL, TOPK).astype(jnp.int32)


def levels(own_key, shape, cuts, smallest, high):
    level, own = 1.0, jax.random.fold_in(own_key, 6)
    for dim, shards_of in cuts:
        heights = jnp.exp(jax.random.uniform(jax.random.fold_in(own, dim), (shards_of,), jnp.float32, smallest / len(cuts), high / len(cuts)))
        level = level * jnp.repeat(heights, shape[dim] // shards_of).reshape([-1 if axis == dim else 1 for axis in range(len(shape))])
    return level


def setup_inputs(seed: int = 0) -> dict:
    key_list = jax.random.split(jax.random.key(seed), 5)
    hidden_states = draw_hidden_states(jax.random.fold_in(key_list[4], 71), 0)
    factor_values = jnp.clip(0.029907227 + 0.10974121 * jax.random.uniform(key_list[1], (POOL, TOPK), jnp.float32) ** levels(key_list[1], (POOL, TOPK), ((0, 16), (1, 8)), -0.2, 0.2), 0.029907227, 0.13964844).astype(jnp.bfloat16)
    class_ids = draw_class_ids(jax.random.fold_in(key_list[4], 71), 0)
    centers = jax.random.randint(key_list[3], (STEPS,), 0, POOL).astype(jnp.int32)
    return {"hidden_states": hidden_states, "factor_values": factor_values, "class_ids": class_ids, "centers": centers}


def reference(hidden_states, factor_values, class_ids, centers):
    nblk = TOPK // K_LOC
    vals = factor_values.astype(jnp.float32)
    sq_h = jnp.sum(jnp.square(hidden_states.astype(jnp.float32)), axis=1)
    sq_a = jnp.sum(vals * vals, axis=1)
    groups = POOL // SAMP_DEV
    means = []
    min_distance = None
    for step in range(STEPS):
        center = centers[step].astype(jnp.int32)
        h_row = lax.dynamic_slice_in_dim(hidden_states, center, 1, 0)[0]
        v_row = lax.dynamic_slice_in_dim(vals, center, 1, 0)[0]
        i_row = lax.dynamic_slice_in_dim(class_ids, center, 1, 0)[0]
        inner_h = jnp.dot(hidden_states, h_row, preferred_element_type=jnp.float32)

        def block(pair):
            values, idents = pair
            match = idents.reshape(-1, nblk, K_LOC, 1) == i_row.reshape(1, nblk, 1, K_LOC)
            prod = values.reshape(-1, nblk, K_LOC, 1) * v_row.reshape(1, nblk, 1, K_LOC)
            return jnp.sum(jnp.where(match, prod, jnp.float32(0.0)), axis=(1, 2, 3))

        inner_a = lax.map(block, (vals.reshape(groups, SAMP_DEV, TOPK), class_ids.reshape(groups, SAMP_DEV, TOPK))).reshape(POOL)
        norm_hc = jnp.sum(jnp.square(h_row.astype(jnp.float32)))
        norm_ac = jnp.sum(v_row * v_row)
        dist = jnp.maximum(sq_h * sq_a + norm_hc * norm_ac - 2.0 * inner_h * inner_a, jnp.float32(0.0))
        min_distance = dist if step == 0 else jnp.minimum(min_distance, dist)
        means.append(jnp.sum(min_distance) / POOL)
    return min_distance, jnp.stack(means)
```

```python
import functools

import jax
import jax.numpy as jnp
from jax import lax
from jax.experimental import pallas as pl
from jax.experimental.pallas import tpu as pltpu
from jax.sharding import PartitionSpec as P

MESH = pl.DeviceIdType.MESH
STEPS = 3
LANES = 128
TALL = 16
CHUNKS = 8
VOCAB = 128256
NT = (((1,), (1,)), ((), ()))
NN = (((1,), (0,)), ((), ()))
DP_ORDER = (13, 12, 15, 11, 14, 10, 9, 5, 8, 4, 7, 3, 6, 2, 1)
MP_ORDER = (5, 4, 7, 3, 6, 2, 1)


def partner(p, k):
    bit = 1
    q = p
    while bit <= k:
        if k & bit:
            q = q + bit - 2 * bit * lax.rem(lax.div(p, bit), 2)
        bit *= 2
    return q


def drain(ref, sem):
    pltpu.make_async_copy(ref, ref, sem).wait()


def encode(k, base):
    local = k - base
    high = local >> 7
    x = (local & 127).astype(jnp.float32) * (1.0 / 128.0) + 1.0
    for j in range(7):
        x = jnp.where((high & (1 << j)) != 0, x * (2.0 ** (1 << j)), x)
    return x


def tiled(x):
    rows, depth = x.shape
    return x.T.reshape(depth // 8, 8, rows // LANES, LANES).transpose(0, 2, 1, 3)


def finish(low_ref, mean_ref, dist_ref, means_ref):
    dist_ref[...] = low_ref[...]
    means_ref[...] = mean_ref[0:STEPS]


def kernel(DP, MP, *refs):
    h = refs[7]
    width = h.shape[2]
    rows = h.shape[0] * h.shape[1]
    depth = refs[9].shape[0] * refs[9].shape[2]
    tiles = rows // LANES
    pl.run_scoped(
        functools.partial(steps, DP, MP, *refs),
        pltpu.VMEM((tiles, width, LANES), jnp.bfloat16),
        pltpu.VMEM((tiles, depth, LANES), jnp.bfloat16),
        pltpu.VMEM((STEPS * 2 * depth, depth, LANES), jnp.bfloat16),
    )


def steps(
    DP, MP,
    c_hbm, h_hbm, v_hbm, i_hbm,
    dist_ref, mean_ref,
    c_ref, h, v, ids, vals, ch_buf, ch_slots, sq, sq_slots, part, own_ref, part_slots,
    row_buf, row_slots,
    z_sem, h_sem, i_sem, v_sem, a_send, a_recv, s_send, s_recv, b_send, b_recv,
    d_send, d_recv, flip, code, splat,
):
    groups, tall, width = h.shape
    rows = groups * tall
    halves = ids.shape[0]
    depth = halves * ids.shape[2]
    blk = rows // MP
    my_dp = lax.axis_index("dp")
    my_mp = lax.axis_index("mp")
    me = my_dp * MP + my_mp
    f32, bf16 = jnp.float32, jnp.bfloat16
    dp_peers = [partner(my_dp, k) for k in range(DP)]
    mp_peers = [partner(my_mp, k) for k in range(MP)]

    step = max(groups // CHUNKS, 1)
    for j in range(0, groups, step):
        at = pl.ds(j, step)
        pltpu.make_async_copy(h_hbm.at[at], h.at[at], h_sem).start()
    pltpu.make_async_copy(c_hbm, c_ref, z_sem).start()
    pltpu.make_async_copy(i_hbm, ids, i_sem).start()
    pltpu.make_async_copy(v_hbm, v, v_sem).start()
    barrier = pltpu.get_barrier_semaphore()
    for k in DP_ORDER:
        pl.semaphore_signal(barrier, inc=1, device_id=(dp_peers[k], my_mp), device_id_type=MESH)
    for k in MP_ORDER:
        pl.semaphore_signal(barrier, inc=1, device_id=(my_dp, mp_peers[k]), device_id_type=MESH)

    pltpu.make_async_copy(c_hbm, c_ref, z_sem).wait()
    drain(ids, i_sem)
    drain(v, v_sem)

    base = my_mp * (VOCAB // MP)
    lane = lax.broadcasted_iota(jnp.int32, (2 * depth, LANES), 1)
    row16 = lax.broadcasted_iota(jnp.int32, (tall, 1), 0)
    ones = jnp.ones((8, LANES), bf16)
    first = my_dp * rows
    offs = [lax.rem(c_ref[t], rows) for t in range(STEPS)]
    found = []
    for t in range(STEPS):
        g = lax.div(offs[t], LANES)
        own = [ids[i, g] for i in range(halves)] + [v[i, g].astype(f32) for i in range(halves)]
        own[:halves] = [encode(x, base) for x in own[:halves]]
        both = jnp.concatenate(own, axis=0)
        hit = lane + (first + g * LANES) == c_ref[t]
        found.append(jnp.where(hit, both, 0.0))
    found.append(jnp.zeros((LANES - STEPS * 2 * depth, LANES), f32))
    meta = lax.dot_general(
        ones, jnp.concatenate(found, axis=0).astype(bf16), NT, preferred_element_type=f32
    )[0:1]
    meta = jnp.concatenate([meta, jnp.zeros((1, width - LANES), f32)], axis=1)
    drain(h, h_sem)
    picks = []
    for t in range(STEPS):
        g = lax.div(offs[t], tall)
        hit = row16 + (first + g * tall) == c_ref[t]
        picks.append(jnp.sum(jnp.where(hit, h[g].astype(f32), 0.0), axis=0, keepdims=True))
    picks.append(meta)
    ch_buf[...] = jnp.concatenate(picks, axis=0).astype(bf16)

    pl.semaphore_wait(barrier, DP - 1 + MP - 1)
    for k in DP_ORDER:
        pltpu.make_async_remote_copy(
            src_ref=ch_buf, dst_ref=ch_slots.at[k - 1], send_sem=a_send, recv_sem=a_recv,
            device_id=(dp_peers[k], my_mp), device_id_type=MESH,
        ).start()

    tiles = blk // LANES
    for b in range(MP):
        turned = h[b * blk // tall:(b + 1) * blk // tall].reshape(blk, width).T
        for j in range(tiles):
            x = turned[:, j * LANES:(j + 1) * LANES]
            flip[b * tiles + j] = x
            x = x.astype(f32)
            sq[b, 0:1, j * LANES:(j + 1) * LANES] = jnp.sum(x * x, axis=0, keepdims=True)
            at = b * tiles + j
            a = jnp.concatenate([v[i, at].astype(f32) for i in range(halves)], axis=0)
            vals[at] = a
            sq[b, 1:2, j * LANES:(j + 1) * LANES] = jnp.sum(a * a, axis=0, keepdims=True)
            k = jnp.concatenate([ids[i, at] for i in range(halves)], axis=0)
            code[at] = encode(k, base).astype(bf16)
    for k in MP_ORDER:
        pltpu.make_async_remote_copy(
            src_ref=sq.at[mp_peers[k]], dst_ref=sq_slots.at[k - 1], send_sem=s_send, recv_sem=s_recv,
            device_id=(my_dp, mp_peers[k]), device_id_type=MESH,
        ).start()

    drain(ch_slots, a_recv)
    ch4 = ch_buf[...]
    for d in range(DP - 1):
        ch4 = ch4 + ch_slots[d]
    ch4 = ch4.astype(f32)
    row8 = lax.broadcasted_iota(jnp.int32, (8, 1), 0)
    ch8 = jnp.concatenate([ch4, jnp.zeros_like(ch4)], axis=0)
    ch = jnp.where(row8 < STEPS, ch8, 0.0)
    meta = ch4[3:4, 0:LANES]
    nh = jnp.sum(ch * ch, axis=1, keepdims=True)
    lane1 = lax.broadcasted_iota(jnp.int32, (1, LANES), 1)
    ch = jnp.concatenate([ch, jnp.zeros_like(ch)], axis=0).astype(bf16)
    norms = jnp.zeros((1, LANES), f32)
    for t in range(STEPS):
        here = (lane1 >= (2 * t + 1) * depth) & (lane1 < (2 * t + 2) * depth)
        na = jnp.sum(jnp.where(here, meta * meta, 0.0), axis=1, keepdims=True)
        norms = jnp.where(lane1 == t, nh[t:t + 1], norms)
        norms = jnp.where(lane1 == STEPS + t, na, norms)
    norms = jnp.concatenate([norms, jnp.zeros((1, blk - LANES), f32)], axis=1)
    norms_hi = norms.astype(bf16).astype(f32)
    norms_lo = norms - norms_hi
    tail = jnp.where(row8 == 2 * STEPS, norms_hi, jnp.where(row8 == 2 * STEPS + 1, norms_lo, 0.0))
    cols = jnp.broadcast_to(meta, (LANES, LANES)).T
    for r in range(STEPS * 2 * depth):
        splat[r] = jnp.broadcast_to(cols[r:r + 1], (depth, LANES)).astype(bf16)

    for k in MP_ORDER + (0,):
        b = mp_peers[k]
        hb = jnp.concatenate([flip[b * tiles + j] for j in range(tiles)], axis=1)
        total = lax.dot_general(ch, hb, NN, preferred_element_type=f32)[0:8] + tail
        cb = [code[b * tiles + j] for j in range(tiles)]
        for t in range(STEPS):
            w = [jnp.zeros((depth, LANES), bf16) for _ in range(tiles)]
            for l in range(depth):
                kl = splat[2 * depth * t + l]
                vl = splat[2 * depth * t + depth + l]
                for j in range(tiles):
                    w[j] = jnp.where(cb[j] == kl, vl, w[j])
            aa = jnp.concatenate(
                [
                    jnp.sum(vals[b * tiles + j] * w[j].astype(f32), axis=0, keepdims=True)
                    for j in range(tiles)
                ],
                axis=1,
            )
            total = jnp.where(row8 == STEPS + t, aa, total)
        if k:
            part[b] = total.astype(bf16)
            pltpu.make_async_remote_copy(
                src_ref=part.at[b], dst_ref=part_slots.at[k - 1], send_sem=b_send, recv_sem=b_recv,
                device_id=(my_dp, b), device_id_type=MESH,
            ).start()
        else:
            own_ref[...] = total
    own = sq[my_mp]
    drain(sq_slots, s_recv)
    for k in range(MP - 1):
        own = own + sq_slots[k]
    own = own[0:1] * own[1:2]
    total = own_ref[...]
    drain(part_slots, b_recv)
    for k in range(MP - 1):
        total = total + part_slots[k].astype(f32)
    norms = total[2 * STEPS:2 * STEPS + 1] + total[2 * STEPS + 1:2 * STEPS + 2]
    row = jnp.zeros((1, LANES), f32)
    low = None
    for t in range(STEPS):
        cross = total[t:t + 1] * total[STEPS + t:STEPS + t + 1]
        far = own + norms[:, t:t + 1] * norms[:, STEPS + t:STEPS + t + 1]
        dist = jnp.maximum(far - 2.0 * cross, 0.0)
        low = dist if low is None else jnp.minimum(low, dist)
        row = jnp.where(lane1 == t, jnp.sum(low, axis=1, keepdims=True), row)
    row_buf[...] = row
    for kd in DP_ORDER + (0,):
        for km in MP_ORDER + (0,):
            if kd or km:
                pltpu.make_async_remote_copy(
                    src_ref=row_buf, dst_ref=row_slots.at[pl.ds(me, 1)],
                    send_sem=d_send, recv_sem=d_recv,
                    device_id=(dp_peers[kd], mp_peers[km]), device_id_type=MESH,
                ).start()
    row_slots[pl.ds(me, 1), :] = row
    dist_ref[...] = low
    drain(ch_slots, a_send)
    drain(sq_slots, s_send)
    drain(part_slots, b_send)
    others = row_slots.at[pl.ds(0, DP * MP - 1)]
    drain(others, d_send)
    drain(others, d_recv)
    mean_ref[...] = jnp.sum(row_slots[...], axis=0, keepdims=True) / (blk * MP * DP)


def solution(mesh):
    DP, MP = mesh.shape["dp"], mesh.shape["mp"]

    def body(hidden_states, factor_values, class_ids, centers):
        rows, width = hidden_states.shape
        depth = class_ids.shape[1]
        blk = rows // MP
        vm = pltpu.VMEM
        sem = pltpu.SemaphoreType.DMA
        hbm = pl.BlockSpec(memory_space=pl.ANY)
        low, mean = pl.pallas_call(
            functools.partial(kernel, DP, MP),
            out_shape=(vm((1, blk), jnp.float32), vm((1, LANES), jnp.float32)),
            in_specs=[hbm] * 4,
            out_specs=(pl.BlockSpec(memory_space=vm), pl.BlockSpec(memory_space=vm)),
            scratch_shapes=[
                pltpu.SMEM((STEPS,), jnp.int32),
                vm((rows // TALL, TALL, width), jnp.bfloat16),
                vm((depth // 8, rows // LANES, 8, LANES), jnp.bfloat16),
                vm((depth // 8, rows // LANES, 8, LANES), jnp.int32),
                vm((rows // LANES, depth, LANES), jnp.float32),
                vm((4, width), jnp.bfloat16),
                vm((DP - 1, 4, width), jnp.bfloat16),
                vm((MP, 2, blk), jnp.float32),
                vm((MP - 1, 2, blk), jnp.float32),
                vm((MP, 8, blk), jnp.bfloat16),
                vm((8, blk), jnp.float32),
                vm((MP - 1, 8, blk), jnp.bfloat16),
                vm((1, LANES), jnp.float32),
                vm((DP * MP, LANES), jnp.float32),
                *[sem] * 12,
            ],
            compiler_params=pltpu.CompilerParams(collective_id=0, has_side_effects=True),
        )(
            centers, hidden_states.reshape(rows // TALL, TALL, width),
            tiled(factor_values), tiled(class_ids),
        )
        spec = pl.BlockSpec(memory_space=vm)
        return pl.pallas_call(
            finish,
            out_shape=(
                jax.ShapeDtypeStruct((blk,), jnp.float32),
                jax.ShapeDtypeStruct((STEPS,), jnp.float32),
            ),
            in_specs=[spec, spec],
            out_specs=(spec, spec),
        )(
            pltpu.with_memory_space_constraint(low.reshape(blk), vm),
            pltpu.with_memory_space_constraint(mean.reshape(LANES), vm),
        )

    return jax.shard_map(
        body,
        mesh=mesh,
        in_specs=(P("dp", "mp"), P("dp", "mp"), P("dp", "mp"), P()),
        out_specs=(P(("dp", "mp")), P()),
        check_vma=False,
    )
```
